32 devices in a mesh: groups: 2 (over y), seq: 4 (over z), head: 2 (over x), rep: 2 (over core).
Axes of the slice: x: 2, y: 2, z: 4, core: 2. Of those that a mesh axis runs over, the one named last changes fastest.
Arguments:
- queries: bfloat16 [128, 64, 128], P(('groups', 'seq', 'rep'), 'head'), parts along dimension 0, may hold values from -256 to 256
- page_owner: int32 [128, 128], P(('groups', 'seq', 'rep')), parts along dimension 0, may hold values from -1 to 3, as said below
- page_slot: int32 [128, 128], P(('groups', 'seq', 'rep')), parts along dimension 0, may hold values from -1 to 63, as said below
- lengths: int32 [128], P(('groups', 'seq', 'rep')), parts along dimension 0, may hold values from 1 to 16384, as said below
- keys: bfloat16 [1024, 8, 128, 128], P(('groups', 'seq', 'rep'), 'head'), parts along dimension 0, may hold values from -24 to 24
- values: bfloat16 [1024, 8, 128, 128], P(('groups', 'seq', 'rep'), 'head'), parts along dimension 0, may hold values from -6 to 6
Outputs:
- attended: bfloat16 [128, 64, 128], P(('groups', 'seq', 'rep'), 'head'), parts along dimension 0
The draws below stay inside these ranges and needn't reach their ends.
There are 2 independent parts, one for each index of `groups`. The reference program is written for one: setup_inputs(seed, part) draws one part's arguments, and reference() takes and returns one part's arrays. A program takes and returns all parts, laid end to end along the dimension named above; each array names one. Nothing has to cross between parts.
Inputs may be any that keep to these rules, and one draw needn't show every extreme that they name: `page_owner`: for j below ceil(lengths[r] / 128) the seq index of the device, among those of r's half (r // 8) % 2, whose pool holds page j of r; -1 for later j. `page_slot`: the page's slot in that pool, -1 where page_owner is -1. No slot of a pool holds two pages; in each half, some device's pool has all 64 slots in use. `lengths`: in each half some request has the most.
All inputs are finite; a program needn't handle non-finite values.
Results may differ from the reference program's by a relative error of at most 0.0041.
Values may be sent and summed in bfloat16 or wider, within the bound.
A program may use at most 64 MiB of HBM per device.

```python
import math
import jax
import jax.numpy as jnp
from jax import lax

QH = 64
KVH = 8
HD = 128
PAGE = 128
MAXP = 128
REQ_DEV = 8
POOL_DEV = 64
REQ = 64
N_SEQ = 4
N_REP = 2


def page_layout(key):
    rows_half = REQ_DEV * N_SEQ
    total_pages = POOL_DEV * (N_SEQ + 1) // 2
    spare_pages = total_pages - rows_half
    extra_cells = rows_half * (MAXP - 1)
    slots_all = N_SEQ * POOL_DEV
    owner_list = []
    slot_list = []
    length_list = []
    for half_index in range(N_REP):
        half_keys = jax.random.split(jax.random.fold_in(key, 101 + half_index), 6)
        longest = jax.random.randint(half_keys[0], (), 0, rows_half)
        shuffled = jax.random.permutation(half_keys[1], extra_cells).astype(jnp.int32)
        cell_row = jnp.arange(extra_cells, dtype=jnp.int32) // (MAXP - 1)
        priority = jnp.where(cell_row == longest, shuffled - extra_cells, shuffled)
        ranked = jnp.argsort(priority)
        chosen = jnp.zeros((extra_cells,), jnp.int32).at[ranked[:spare_pages]].set(1)
        page_count = 1 + jnp.sum(chosen.reshape(rows_half, MAXP - 1), axis=1)
        tail_tokens = jax.random.randint(half_keys[2], (rows_half,), 1, PAGE + 1)
        tail_tokens = jnp.where(jnp.arange(rows_half) == longest, PAGE, tail_tokens)
        length_list.append((page_count - 1) * PAGE + tail_tokens)
        device_weight = jax.random.randint(half_keys[3], (N_SEQ,), 2, 5)
        lightest = jax.random.randint(half_keys[4], (), 0, N_SEQ)
        device_weight = jnp.where(jnp.arange(N_SEQ) == lightest, 1, device_weight)
        tie_break = jax.random.permutation(half_keys[5], slots_all).astype(jnp.int32)
        slot_ids = jnp.arange(slots_all, dtype=jnp.int32)
        slot_score = slot_ids % POOL_DEV * device_weight[slot_ids // POOL_DEV] * slots_all + tie_break
        picked = jnp.argsort(slot_score)[:total_pages].astype(jnp.int32)
        first_page = jnp.cumsum(page_count) - page_count
        page_index = jnp.arange(MAXP, dtype=jnp.int32)
        page_used = page_index[None, :] < page_count[:, None]
        flat_index = jnp.clip(first_page[:, None] + page_index[None, :], 0, total_pages - 1)
        chosen_slot = picked[flat_index]
        owner_list.append(jnp.where(page_used, chosen_slot // POOL_DEV, -1))
        slot_list.append(jnp.where(page_used, chosen_slot % POOL_DEV, -1))

    def arrange(pieces):
        tail_shape = pieces[0].shape[1:]
        stacked = jnp.stack(pieces).reshape((N_REP, N_SEQ, REQ_DEV) + tail_shape)
        stacked = jnp.moveaxis(stacked, 0, 1)
        return stacked.reshape((REQ,) + tail_shape).astype(jnp.int32)
    return (arrange(owner_list), arrange(slot_list), arrange(length_list))


def draw_page_owner(key, part):
    return page_layout(key)[0]


def draw_page_slot(key, part):
    return page_layout(key)[1]


def draw_lengths(key, part):
    return page_layout(key)[2]


def draw_keys(key, part):
    full_shape = (N_SEQ * N_REP * POOL_DEV, KVH, PAGE, HD)
    sample = jax.random.normal(jax.random.fold_in(key, 11), full_shape, jnp.float32)
    return jnp.clip(sample, -24.0, 24.0).astype(jnp.bfloat16)


def draw_queries(key, part):
    full_shape = (REQ, QH, HD)
    sample = jax.random.normal(jax.random.fold_in(key, 23), full_shape, jnp.float32)
    return jnp.clip(sample, -256.0, 256.0).astype(jnp.bfloat16)


def levels(rng, dims, cuts, least, top_value):
    gain = 1.0
    for dim, shards_of in cuts:
        heights = jax.random.uniform(jax.random.fold_in(jax.random.fold_in(rng, 6), dim), (shards_of,), jnp.float32, least / len(cuts), top_value / len(cuts))
        gain = gain * jnp.repeat(jnp.exp(heights), dims[dim] // shards_of).reshape((-1,) + (1,) * (len(dims) - 1 - dim))
    return gain


def bell_draw(stream_key, dims, scale, bound, cuts=(), kind=jnp.bfloat16):
    result = jax.random.normal(stream_key, dims, jnp.float32) * scale
    if len(cuts) > 0:
        result = levels(stream_key, dims, cuts, -0.22, 0.18) * result
    return jnp.clip(result, min=-bound, max=bound).astype(kind)


def setup_inputs(seed: int = 0, part: int = 0) -> dict:
    key_of = jax.random.split(jax.random.key(seed), 7)
    part_splits = jax.random.split(jax.random.fold_in(key_of[6], part), 7)
    queries = draw_queries(jax.random.fold_in(jax.random.fold_in(key_of[6], part), 71), part)
    page_owner = draw_page_owner(jax.random.fold_in(jax.random.fold_in(key_of[6], part), 71), part)
    page_slot = draw_page_slot(jax.random.fold_in(jax.random.fold_in(key_of[6], part), 71), part)
    lengths = draw_lengths(jax.random.fold_in(jax.random.fold_in(key_of[6], part), 71), part)
    keys = draw_keys(jax.random.fold_in(jax.random.fold_in(key_of[6], part), 71), part)
    values = bell_draw(part_splits[5], (N_SEQ * N_REP * POOL_DEV, KVH, PAGE, HD), 1.0, 6.0, ((0, 8), (1, 2)))
    return {"queries": queries, "page_owner": page_owner, "page_slot": page_slot, "lengths": lengths, "keys": keys, "values": values}


masked_score = -1e+30

def reference(queries, page_owner, page_slot, lengths, keys, values):
    request_count = queries.shape[0]
    group_size = QH // KVH
    score_scale = 1.0 / math.sqrt(HD)
    half_index = (jnp.arange(request_count, dtype=jnp.int32) // REQ_DEV % N_REP).astype(jnp.int32)
    page_index = jnp.arange(MAXP, dtype=jnp.int32)
    token_index = jnp.arange(PAGE, dtype=jnp.int32)

    def attend_one(request_data):
        single_query, owner_row, slot_row, token_count, half_side = request_data
        pool_index = ((jnp.maximum(owner_row, 0) * N_REP + half_side) * POOL_DEV + jnp.maximum(slot_row, 0)).astype(jnp.int32)
        page_keys = keys[pool_index].astype(jnp.float32)
        page_values = values[pool_index].astype(jnp.float32)
        grouped_query = single_query.astype(jnp.float32).reshape(KVH, group_size, HD)
        scores = jnp.einsum('kgd,jktd->jkgt', grouped_query, page_keys, precision=lax.Precision.HIGHEST) * score_scale
        live_count = jnp.clip(token_count - page_index * PAGE, 0, PAGE)
        live_tokens = (token_index[None, :] < live_count[:, None])[:, None, None, :]
        scores = jnp.where(live_tokens, scores, masked_score)
        page_max = lax.optimization_barrier(jnp.max(scores, axis=3))
        weights = jnp.where(live_tokens, jnp.exp(scores - page_max[..., None]), 0.0)
        page_sum = lax.optimization_barrier(jnp.sum(weights, axis=3))
        rounded = lax.optimization_barrier(weights.astype(jnp.bfloat16))
        page_out = jnp.einsum('jkgt,jktd->jkgd', rounded.astype(jnp.float32), page_values, precision=lax.Precision.HIGHEST)
        live_pages = (live_count > 0)[:, None, None]
        request_top = lax.optimization_barrier(jnp.max(jnp.where(live_pages, page_max, masked_score), axis=0))
        rescale = jnp.where(live_pages, jnp.exp(jnp.minimum(page_max - request_top[None], 0.0)), 0.0)
        request_total = lax.optimization_barrier(jnp.sum(rescale * page_sum, axis=0))
        request_out = lax.optimization_barrier(jnp.sum(rescale[..., None] * page_out, axis=0))
        return (request_out / request_total[..., None]).astype(jnp.bfloat16).reshape(QH, HD)
    return lax.map(attend_one, (queries, page_owner, page_slot, lengths, half_index))
```

```python
import functools
import math

import jax
import jax.numpy as jnp
from jax import lax
from jax.experimental import pallas as pl
from jax.experimental.pallas import tpu as pltpu
from jax.sharding import PartitionSpec as P

MASKED = -1e30
F32 = jnp.float32
BF16 = jnp.bfloat16
NT = (((1,), (1,)), ((), ()))


def iota(shape, dim):
    return lax.broadcasted_iota(jnp.int32, shape, dim)


def kernel(
    n, unroll, lens_ref, q_ref, owner_ref, slot_ref, k_hbm, v_hbm, out_ref,
    kbuf, vbuf, qall, tsend, trecv, liveb, reqb, mt, m, qslot, pmb, lb, oacc, ohi,
    osend, orecv, ssend, srecv,
    ksem, vsem, tss, trs, qss, qrs, oss, ors, sss, srs,
):
    pool, kv, tokens, width = k_hbm.shape
    rows = q_ref.shape[0]
    group = q_ref.shape[1] // kv
    block = rows * group
    lanes = trecv.shape[2]
    scale = 1.0 / math.sqrt(width)
    me = lax.axis_index("seq")

    def peer(off):
        return {"seq": lax.rem(me + off, n)}

    def source(off):
        return {"seq": lax.rem(me + n - off, n)}

    def remote(src, dst, ssem, rsem, to):
        return pltpu.make_async_remote_copy(
            src_ref=src, dst_ref=dst, send_sem=ssem, recv_sem=rsem,
            device_id=to, device_id_type=pl.DeviceIdType.MESH,
        )

    barrier = pltpu.get_barrier_semaphore()
    for off in range(1, n):
        pl.semaphore_signal(
            barrier, inc=1, device_id=peer(off), device_id_type=pl.DeviceIdType.MESH
        )
    kcopies = [pltpu.make_async_copy(k_hbm.at[:, h], kbuf.at[h], ksem.at[h]) for h in range(kv)]
    vcopies = [pltpu.make_async_copy(v_hbm.at[:, h], vbuf.at[h], vsem.at[h]) for h in range(kv)]
    for h in range(kv):
        kcopies[h].start()
        vcopies[h].start()

    queries = q_ref[...].astype(F32).reshape(rows, kv, group, width)
    for h in range(kv):
        qall[h, 0:block, :] = queries[:, h].reshape(block, width).astype(BF16)

    span = owner_ref.shape[1]
    row = iota((rows, span), 0)
    length = jnp.zeros((rows, span), jnp.int32)
    for r in range(rows):
        length = jnp.where(row == r, lens_ref[r], length)
    live = jnp.clip(length - iota((rows, span), 1) * tokens, 0, tokens)
    live_f = live.astype(F32)
    owner = owner_ref[...]
    slot = slot_ref[...]
    ones = jnp.ones((8, span), BF16)
    slot_id = iota((pool, span), 0)
    for off in range(n):
        there = lax.rem(me + off, n)
        key = jnp.where((owner == there) & (live > 0), slot, -1)
        acc_live = jnp.zeros((pool, span), F32)
        acc_req = jnp.zeros((pool, span), F32)
        for r in range(rows):
            hit = slot_id == key[r : r + 1, :]
            acc_live = jnp.where(hit, live_f[r : r + 1, :], acc_live)
            acc_req = jnp.where(hit, float(r + 1), acc_req)
        t_live = lax.dot_general(ones, acc_live.astype(BF16), NT, preferred_element_type=F32)
        t_req = lax.dot_general(ones, acc_req.astype(BF16), NT, preferred_element_type=F32)
        table = jnp.where(iota((8, pool), 0) == 0, t_live, t_req)
        if lanes > pool:
            table = jnp.concatenate([table, jnp.zeros((8, lanes - pool), F32)], axis=1)
        if off == 0:
            trecv[0] = table
        else:
            tsend[off] = table

    pl.semaphore_wait(barrier, n - 1)
    tcopies = {}
    qcopies = {}
    for off in range(1, n):
        tcopies[off] = remote(
            tsend.at[off], trecv.at[off], tss.at[off], trs.at[off], peer(off)
        )
        tcopies[off].start()
    for h in range(kv):
        for off in range(1, n):
            qcopies[h, off] = remote(
                qall.at[h, pl.ds(0, block)],
                qall.at[h, pl.ds(off * block, block)],
                qss.at[h, off], qrs.at[h, off], peer(off),
            )
            qcopies[h, off].start()

    for off in range(1, n):
        tcopies[off].wait_recv()
    live_row = trecv[0][0:1, :]
    req_row = trecv[0][1:2, :]
    for off in range(1, n):
        t = trecv[off]
        live_row = live_row + t[0:1, :]
        req_row = req_row + jnp.where(t[1:2, :] > 0.0, t[1:2, :] + float(off * rows), 0.0)
    pg = pool * group
    spread = jnp.where(iota((pg, lanes), 0) // group == iota((pg, lanes), 1), 1.0, 0.0)
    spread = spread.astype(BF16)
    liveb[...] = lax.dot_general(
        spread, jnp.broadcast_to(live_row, (128, lanes)).astype(BF16), NT,
        preferred_element_type=F32,
    )
    reqb[...] = lax.dot_general(
        spread, jnp.broadcast_to(req_row, (128, lanes)).astype(BF16), NT,
        preferred_element_type=F32,
    )
    same = iota((pg, 128), 0) % group == iota((pg, 128), 1) % group
    for c in range(n * block // 128):
        want = ((iota((pg, 128), 1) + c * 128) // group + 1).astype(F32)
        mt[:, c * 128 : (c + 1) * 128] = jnp.where(
            same & (reqb[...] == want), 1.0, 0.0
        ).astype(BF16)
    spread_t = jnp.where(iota((lanes, pg), 0) == iota((lanes, pg), 1) // group, 1.0, 0.0)
    req_wide = jnp.dot(
        jnp.broadcast_to(req_row, (8, lanes)).astype(BF16), spread_t.astype(BF16),
        preferred_element_type=F32,
    )[0:1, :]
    same_t = iota((block, pg), 0) % group == iota((block, pg), 1) % group
    for off in range(n):
        want = (iota((block, pg), 0) // group + (off * rows + 1)).astype(F32)
        m[off * block : (off + 1) * block, :] = jnp.where(
            same_t & (req_wide == want), 1.0, 0.0
        ).astype(BF16)

    lane_f = iota((group, 128), 1).astype(F32)
    tops = []
    sums = []
    ocopies = {}
    for h in range(kv):
        for off in range(1, n):
            qcopies[h, off].wait_recv()
        qslot[...] = jnp.dot(mt[...], qall[h], preferred_element_type=F32)
        kcopies[h].wait()
        vcopies[h].wait()

        def pages(i, top):
            for u in range(unroll):
                p = i * unroll + u
                at = pl.ds(pl.multiple_of(p * group, group), group)
                s = lax.dot_general(
                    qslot[at, :].astype(BF16), kbuf[h, p], NT, preferred_element_type=F32
                )
                s = jnp.where(lane_f < liveb[at, :], s * scale, MASKED)
                pm = jnp.max(s, axis=1, keepdims=True)
                w = jnp.exp(s - pm)
                total = jnp.sum(w, axis=1, keepdims=True)
                oacc[at, :] = jnp.dot(w.astype(BF16), vbuf[h, p], preferred_element_type=F32)
                pmb[at, :] = jnp.broadcast_to(pm, (group, 128))
                lb[at, :] = jnp.broadcast_to(total, (group, 128))
                top = jnp.maximum(top, jnp.where(reqb[at, :] == lane_f + 1.0, pm, MASKED))
            return top

        top = lax.fori_loop(0, pool // unroll, pages, jnp.full((group, 128), MASKED, F32))

        def merge(i, acc):
            for u in range(unroll):
                p = i * unroll + u
                at = pl.ds(pl.multiple_of(p * group, group), group)
                mine = reqb[at, :] == lane_f + 1.0
                rm = jnp.max(jnp.where(mine, top, MASKED), axis=1, keepdims=True)
                sc = jnp.exp(jnp.minimum(pmb[at, :] - rm, 0.0))
                ohi[at, :] = oacc[at, :] * sc
                acc = acc + jnp.where(mine, sc * lb[at, :], 0.0)
            return acc

        acc = lax.fori_loop(0, pool // unroll, merge, jnp.zeros((group, 128), F32))
        osend[h] = jnp.dot(
            m[...], ohi[...].astype(BF16), preferred_element_type=F32
        ).astype(BF16)
        for off in range(1, n):
            ocopies[h, off] = remote(
                osend.at[h, pl.ds(off * block, block)], orecv.at[h, off],
                oss.at[h, off], ors.at[h, off], source(off),
            )
            ocopies[h, off].start()
        tops.append(top)
        sums.append(acc)

    lane = iota((group, 128), 1)
    scopies = {}
    for off in range(n):
        stat = jnp.zeros((group, 128), F32)
        for h in range(kv):
            for j, x in enumerate((tops[h], sums[h])):
                at = (2 * h + j) * rows
                shift = (at - off * rows) % 128
                y = pltpu.roll(x, shift, 1) if shift else x
                stat = jnp.where((lane >= at) & (lane < at + rows), y, stat)
        if off == 0:
            srecv[0] = stat
        else:
            ssend[off] = stat
            scopies[off] = remote(
                ssend.at[off], srecv.at[off], sss.at[off], srs.at[off], source(off)
            )
            scopies[off].start()

    for off in range(1, n):
        scopies[off].wait_recv()
    stats = [srecv[off] for off in range(n)]
    best = functools.reduce(jnp.maximum, stats)
    factors = [jnp.exp(x - best) for x in stats]
    whole = functools.reduce(
        jnp.add, [f * pltpu.roll(x, 128 - rows, 1) for f, x in zip(factors, stats)]
    )
    factors = [f / whole for f in factors]
    parts = []
    for h in range(kv):
        gathered = []
        for off in range(n):
            if off == 0:
                got = osend[h, 0:block, :]
            else:
                ocopies[h, off].wait_recv()
                got = orecv[h, off]
            gathered.append(got.astype(F32).reshape(rows, group, width))
        per_row = []
        for r in range(rows):
            at = 2 * h * rows + r
            total = factors[0][:, at : at + 1] * gathered[0][r]
            for off in range(1, n):
                total = total + factors[off][:, at : at + 1] * gathered[off][r]
            per_row.append(total)
        parts.append(per_row)
    for r in range(rows):
        out_ref[r] = jnp.concatenate([parts[h][r] for h in range(kv)], axis=0).astype(BF16)

    for off in range(1, n):
        tcopies[off].wait_send()
        scopies[off].wait_send()
        for h in range(kv):
            qcopies[h, off].wait_send()
            ocopies[h, off].wait_send()


def on_device(n, queries, page_owner, page_slot, lengths, keys, values):
    pool, kv, tokens, width = keys.shape
    rows, heads, _ = queries.shape
    group = heads // kv
    block = rows * group
    pg = pool * group
    lanes = -(-pool // 128) * 128
    unroll = math.gcd(pool, 16)
    dma = pltpu.SemaphoreType.DMA
    vmem = pl.BlockSpec(memory_space=pltpu.VMEM)
    return pl.pallas_call(
        functools.partial(kernel, n, unroll),
        out_shape=jax.ShapeDtypeStruct(queries.shape, BF16),
        in_specs=[
            pl.BlockSpec(memory_space=pltpu.SMEM),
            vmem,
            vmem,
            vmem,
            pl.BlockSpec(memory_space=pl.ANY),
            pl.BlockSpec(memory_space=pl.ANY),
        ],
        out_specs=vmem,
        scratch_shapes=[
            pltpu.VMEM((kv, pool, tokens, width), BF16),
            pltpu.VMEM((kv, pool, tokens, width), BF16),
            pltpu.VMEM((kv, n * block, width), BF16),
            pltpu.VMEM((n, 8, lanes), F32),
            pltpu.VMEM((n, 8, lanes), F32),
            pltpu.VMEM((pg, 128), F32),
            pltpu.VMEM((pg, 128), F32),
            pltpu.VMEM((pg, n * block), BF16),
            pltpu.VMEM((n * block, pg), BF16),
            pltpu.VMEM((pg, width), F32),
            pltpu.VMEM((pg, 128), F32),
            pltpu.VMEM((pg, 128), F32),
            pltpu.VMEM((pg, width), F32),
            pltpu.VMEM((pg, width), F32),
            pltpu.VMEM((kv, n * block, width), BF16),
            pltpu.VMEM((kv, n, block, width), BF16),
            pltpu.VMEM((n, group, 128), F32),
            pltpu.VMEM((n, group, 128), F32),
            dma((kv,)), dma((kv,)),
            dma((n,)), dma((n,)),
            dma((kv, n)), dma((kv, n)),
            dma((kv, n)), dma((kv, n)),
            dma((n,)), dma((n,)),
        ],
        compiler_params=pltpu.CompilerParams(
            collective_id=0, has_side_effects=True, vmem_limit_bytes=60 * 1024 * 1024
        ),
        name="paged",
    )(lengths, queries, page_owner, page_slot, keys, values)


def solution(mesh):
    placed = (
        P(("groups", "seq", "rep"), "head", None),
        P(("groups", "seq", "rep"), None),
        P(("groups", "seq", "rep"), None),
        P(("groups", "seq", "rep")),
        P(("groups", "seq", "rep"), "head", None, None),
        P(("groups", "seq", "rep"), "head", None, None),
    )
    return jax.shard_map(
        functools.partial(on_device, mesh.shape["seq"]),
        mesh=mesh,
        in_specs=placed,
        out_specs=P(("groups", "seq", "rep"), "head", None),
        check_vma=False,
    )
```

```python
import functools
import math

import jax
import jax.numpy as jnp
from jax import lax
from jax.experimental import pallas as pl
from jax.experimental.pallas import tpu as pltpu
from jax.sharding import PartitionSpec as P

MASKED = -1e30
F32 = jnp.float32
BF16 = jnp.bfloat16
NT = (((1,), (1,)), ((), ()))


def iota(shape, dim):
    return lax.broadcasted_iota(jnp.int32, shape, dim)


def kernel(
    n, unroll, lens_ref, q_ref, owner_ref, slot_ref, k_hbm, v_hbm, out_ref,
    kbuf, vbuf, qall, tsend, trecv, liveb, reqb, mt, m, qslot, pmb, lb, wbuf, ohi,
    osend, orecv, ssend, srecv,
    ksem, vsem, tss, trs, qss, qrs, oss, ors, sss, srs,
):
    pool, kv, tokens, width = k_hbm.shape
    rows = q_ref.shape[0]
    group = q_ref.shape[1] // kv
    block = rows * group
    lanes = trecv.shape[2]
    scale = 1.0 / math.sqrt(width)
    me = lax.axis_index("seq")

    def peer(off):
        return {"seq": lax.rem(me + off, n)}

    def source(off):
        return {"seq": lax.rem(me + n - off, n)}

    def remote(src, dst, ssem, rsem, to):
        return pltpu.make_async_remote_copy(
            src_ref=src, dst_ref=dst, send_sem=ssem, recv_sem=rsem,
            device_id=to, device_id_type=pl.DeviceIdType.MESH,
        )

    barrier = pltpu.get_barrier_semaphore()
    for off in range(1, n):
        pl.semaphore_signal(
            barrier, inc=1, device_id=peer(off), device_id_type=pl.DeviceIdType.MESH
        )
    kcopies = [pltpu.make_async_copy(k_hbm.at[:, h], kbuf.at[h], ksem.at[h]) for h in range(kv)]
    vcopies = [pltpu.make_async_copy(v_hbm.at[:, h], vbuf.at[h], vsem.at[h]) for h in range(kv)]
    for h in range(kv):
        kcopies[h].start()
        vcopies[h].start()

    queries = q_ref[...].astype(F32).reshape(rows, kv, group, width)
    for h in range(kv):
        qall[h, 0:block, :] = queries[:, h].reshape(block, width).astype(BF16)

    span = owner_ref.shape[1]
    row = iota((rows, span), 0)
    length = jnp.zeros((rows, span), jnp.int32)
    for r in range(rows):
        length = jnp.where(row == r, lens_ref[r], length)
    live = jnp.clip(length - iota((rows, span), 1) * tokens, 0, tokens)
    live_f = live.astype(F32)
    owner = owner_ref[...]
    slot = slot_ref[...]
    ones = jnp.ones((8, span), BF16)
    slot_id = iota((pool, span), 0)
    for off in range(n):
        there = lax.rem(me + off, n)
        key = jnp.where((owner == there) & (live > 0), slot, -1)
        acc_live = jnp.zeros((pool, span), F32)
        acc_req = jnp.zeros((pool, span), F32)
        for r in range(rows):
            hit = slot_id == key[r : r + 1, :]
            acc_live = jnp.where(hit, live_f[r : r + 1, :], acc_live)
            acc_req = jnp.where(hit, float(r + 1), acc_req)
        t_live = lax.dot_general(ones, acc_live.astype(BF16), NT, preferred_element_type=F32)
        t_req = lax.dot_general(ones, acc_req.astype(BF16), NT, preferred_element_type=F32)
        table = jnp.where(iota((8, pool), 0) == 0, t_live, t_req)
        if lanes > pool:
            table = jnp.concatenate([table, jnp.zeros((8, lanes - pool), F32)], axis=1)
        if off == 0:
            trecv[0] = table
        else:
            tsend[off] = table

    pl.semaphore_wait(barrier, n - 1)
    tcopies = {}
    qcopies = {}
    for off in range(1, n):
        tcopies[off] = remote(
            tsend.at[off], trecv.at[off], tss.at[off], trs.at[off], peer(off)
        )
        tcopies[off].start()
    for h in range(kv):
        for off in range(1, n):
            qcopies[h, off] = remote(
                qall.at[h, pl.ds(0, block)],
                qall.at[h, pl.ds(off * block, block)],
                qss.at[h, off], qrs.at[h, off], peer(off),
            )
            qcopies[h, off].start()

    for off in range(1, n):
        tcopies[off].wait_recv()
    live_row = trecv[0][0:1, :]
    req_row = trecv[0][1:2, :]
    for off in range(1, n):
        t = trecv[off]
        live_row = live_row + t[0:1, :]
        req_row = req_row + jnp.where(t[1:2, :] > 0.0, t[1:2, :] + float(off * rows), 0.0)
    pg = pool * group
    spread = jnp.where(iota((pg, lanes), 0) // group == iota((pg, lanes), 1), 1.0, 0.0)
    spread = spread.astype(BF16)
    liveb[...] = lax.dot_general(
        spread, jnp.broadcast_to(live_row, (128, lanes)).astype(BF16), NT,
        preferred_element_type=F32,
    )
    reqb[...] = lax.dot_general(
        spread, jnp.broadcast_to(req_row, (128, lanes)).astype(BF16), NT,
        preferred_element_type=F32,
    )
    same = iota((pg, 128), 0) % group == iota((pg, 128), 1) % group
    for c in range(n * block // 128):
        want = ((iota((pg, 128), 1) + c * 128) // group + 1).astype(F32)
        mt[:, c * 128 : (c + 1) * 128] = jnp.where(
            same & (reqb[...] == want), 1.0, 0.0
        ).astype(BF16)
    spread_t = jnp.where(iota((lanes, pg), 0) == iota((lanes, pg), 1) // group, 1.0, 0.0)
    req_wide = jnp.dot(
        jnp.broadcast_to(req_row, (8, lanes)).astype(BF16), spread_t.astype(BF16),
        preferred_element_type=F32,
    )[0:1, :]
    same_t = iota((block, pg), 0) % group == iota((block, pg), 1) % group
    for off in range(n):
        want = (iota((block, pg), 0) // group + (off * rows + 1)).astype(F32)
        m[off * block : (off + 1) * block, :] = jnp.where(
            same_t & (req_wide == want), 1.0, 0.0
        ).astype(BF16)

    lane_f = iota((group, 128), 1).astype(F32)
    tops = []
    sums = []
    ocopies = {}
    for h in range(kv):
        for off in range(1, n):
            qcopies[h, off].wait_recv()
        qslot[...] = jnp.dot(mt[...], qall[h], preferred_element_type=F32)
        kcopies[h].wait()

        def pages(i, top):
            for u in range(unroll):
                p = i * unroll + u
                at = pl.ds(pl.multiple_of(p * group, group), group)
                s = lax.dot_general(
                    qslot[at, :].astype(BF16), kbuf[h, p], NT, preferred_element_type=F32
                )
                s = jnp.where(lane_f < liveb[at, :], s * scale, MASKED)
                pm = jnp.max(s, axis=1, keepdims=True)
                w = jnp.exp(s - pm)
                total = jnp.sum(w, axis=1, keepdims=True)
                wbuf[at, :] = w
                pmb[at, :] = jnp.broadcast_to(pm, (group, 128))
                lb[at, :] = jnp.broadcast_to(total, (group, 128))
                top = jnp.maximum(top, jnp.where(reqb[at, :] == lane_f + 1.0, pm, MASKED))
            return top

        top = lax.fori_loop(0, pool // unroll, pages, jnp.full((group, 128), MASKED, F32))
        vcopies[h].wait()

        def merge(i, acc):
            for u in range(unroll):
                p = i * unroll + u
                at = pl.ds(pl.multiple_of(p * group, group), group)
                out = jnp.dot(wbuf[at, :].astype(BF16), vbuf[h, p], preferred_element_type=F32)
                mine = reqb[at, :] == lane_f + 1.0
                rm = jnp.max(jnp.where(mine, top, MASKED), axis=1, keepdims=True)
                sc = jnp.exp(jnp.minimum(pmb[at, :] - rm, 0.0))
                ohi[at, :] = out * sc
                acc = acc + jnp.where(mine, sc * lb[at, :], 0.0)
            return acc

        acc = lax.fori_loop(0, pool // unroll, merge, jnp.zeros((group, 128), F32))
        osend[h] = jnp.dot(
            m[...], ohi[...].astype(BF16), preferred_element_type=F32
        ).astype(BF16)
        for off in range(1, n):
            ocopies[h, off] = remote(
                osend.at[h, pl.ds(off * block, block)], orecv.at[h, off],
                oss.at[h, off], ors.at[h, off], source(off),
            )
            ocopies[h, off].start()
        tops.append(top)
        sums.append(acc)

    lane = iota((group, 128), 1)
    scopies = {}
    for off in range(n):
        stat = jnp.zeros((group, 128), F32)
        for h in range(kv):
            for j, x in enumerate((tops[h], sums[h])):
                at = (2 * h + j) * rows
                shift = (at - off * rows) % 128
                y = pltpu.roll(x, shift, 1) if shift else x
                stat = jnp.where((lane >= at) & (lane < at + rows), y, stat)
        if off == 0:
            srecv[0] = stat
        else:
            ssend[off] = stat
            scopies[off] = remote(
                ssend.at[off], srecv.at[off], sss.at[off], srs.at[off], source(off)
            )
            scopies[off].start()

    for off in range(1, n):
        scopies[off].wait_recv()
    stats = [srecv[off] for off in range(n)]
    best = functools.reduce(jnp.maximum, stats)
    factors = [jnp.exp(x - best) for x in stats]
    whole = functools.reduce(
        jnp.add, [f * pltpu.roll(x, 128 - rows, 1) for f, x in zip(factors, stats)]
    )
    factors = [f / whole for f in factors]
    parts = []
    for h in range(kv):
        gathered = []
        for off in range(n):
            if off == 0:
                got = osend[h, 0:block, :]
            else:
                ocopies[h, off].wait_recv()
                got = orecv[h, off]
            gathered.append(got.astype(F32).reshape(rows, group, width))
        per_row = []
        for r in range(rows):
            at = 2 * h * rows + r
            total = factors[0][:, at : at + 1] * gathered[0][r]
            for off in range(1, n):
                total = total + factors[off][:, at : at + 1] * gathered[off][r]
            per_row.append(total)
        parts.append(per_row)
    for r in range(rows):
        out_ref[r] = jnp.concatenate([parts[h][r] for h in range(kv)], axis=0).astype(BF16)

    for off in range(1, n):
        tcopies[off].wait_send()
        scopies[off].wait_send()
        for h in range(kv):
            qcopies[h, off].wait_send()
            ocopies[h, off].wait_send()


def on_device(n, queries, page_owner, page_slot, lengths, keys, values):
    pool, kv, tokens, width = keys.shape
    rows, heads, _ = queries.shape
    group = heads // kv
    block = rows * group
    pg = pool * group
    lanes = -(-pool // 128) * 128
    unroll = math.gcd(pool, 16)
    dma = pltpu.SemaphoreType.DMA
    vmem = pl.BlockSpec(memory_space=pltpu.VMEM)
    return pl.pallas_call(
        functools.partial(kernel, n, unroll),
        out_shape=jax.ShapeDtypeStruct(queries.shape, BF16),
        in_specs=[
            pl.BlockSpec(memory_space=pltpu.SMEM),
            vmem,
            vmem,
            vmem,
            pl.BlockSpec(memory_space=pl.ANY),
            pl.BlockSpec(memory_space=pl.ANY),
        ],
        out_specs=vmem,
        scratch_shapes=[
            pltpu.VMEM((kv, pool, tokens, width), BF16),
            pltpu.VMEM((kv, pool, tokens, width), BF16),
            pltpu.VMEM((kv, n * block, width), BF16),
            pltpu.VMEM((n, 8, lanes), F32),
            pltpu.VMEM((n, 8, lanes), F32),
            pltpu.VMEM((pg, 128), F32),
            pltpu.VMEM((pg, 128), F32),
            pltpu.VMEM((pg, n * block), BF16),
            pltpu.VMEM((n * block, pg), BF16),
            pltpu.VMEM((pg, width), F32),
            pltpu.VMEM((pg, 128), F32),
            pltpu.VMEM((pg, 128), F32),
            pltpu.VMEM((pg, width), F32),
            pltpu.VMEM((pg, width), F32),
            pltpu.VMEM((kv, n * block, width), BF16),
            pltpu.VMEM((kv, n, block, width), BF16),
            pltpu.VMEM((n, group, 128), F32),
            pltpu.VMEM((n, group, 128), F32),
            dma((kv,)), dma((kv,)),
            dma((n,)), dma((n,)),
            dma((kv, n)), dma((kv, n)),
            dma((kv, n)), dma((kv, n)),
            dma((n,)), dma((n,)),
        ],
        compiler_params=pltpu.CompilerParams(
            collective_id=0, has_side_effects=True, vmem_limit_bytes=60 * 1024 * 1024
        ),
        name="paged",
    )(lengths, queries, page_owner, page_slot, keys, values)


def solution(mesh):
    placed = (
        P(("groups", "seq", "rep"), "head", None),
        P(("groups", "seq", "rep"), None),
        P(("groups", "seq", "rep"), None),
        P(("groups", "seq", "rep")),
        P(("groups", "seq", "rep"), "head", None, None),
        P(("groups", "seq", "rep"), "head", None, None),
    )
    return jax.shard_map(
        functools.partial(on_device, mesh.shape["seq"]),
        mesh=mesh,
        in_specs=placed,
        out_specs=P(("groups", "seq", "rep"), "head", None),
        check_vma=False,
    )
```
